32 devices in a mesh: frag: 8 (over z, y), blk: 4 (over x, core).
Axes of the slice: x: 2, y: 2, z: 4, core: 2. Of those that a mesh axis runs over, the one named last changes fastest.
Arguments:
- amps: float32 [8, 128, 8, 128], P('frag', 'blk'), may hold values from -1.5 to 1.5
- exch: float32 [8, 128, 8, 128], P('frag', 'blk'), may hold values from -4 to 4
- factors: bfloat16 [8, 384, 128, 128], P('frag', 'blk'), may hold values from -0.109375 to 0.109375
- occupied_pair_ladder: float32 [8, 8, 8], P('frag'), may hold values from -1 to 1
- virtual_fock_block: float32 [8, 128, 128], P('frag'), may hold values from -0.1875 to 0.1875
- virtual_orbital_energy: float32 [8, 128], P('frag'), may hold values from 1 to 3
- pair_energy: float32 [8, 8], P('frag'), may hold values from -1.5 to -0.5
- energy_weight: int32 [8, 8], P('frag'), may hold values from 0 to 2
- export_rows: int32 [8, 2, 2], P('frag'), may hold values from 2 to 5, as said below
Outputs:
- new_amps: float32 [8, 128, 8, 128], P('frag', 'blk')
- res_norms: float32 [8, 2], P('frag')
- energy: float32 [], replicated
The draws below stay inside these ranges and needn't reach their ends.
Inputs may be any that keep to these rules, and one draw needn't show every extreme that they name: `export_rows`: for each fragment the 4 entries are distinct core rows.
All inputs are finite; a program needn't handle non-finite values.
Results may differ from the reference program's by a relative error of at most 0.0009.
Values may be sent and summed in bfloat16 or wider, within the bound.
A program may use at most 128 MiB of HBM per device.

```python
import math
import jax
import jax.numpy as jnp
from jax import lax

V = 128
NAUX = 384
P_SIZE = 8
BUF = 2
PASSES = 2
FRAGS = 8


def fragment_rows(key):
    chosen = jax.random.permutation(key, P_SIZE - 2 * BUF)[:2 * BUF]
    return (chosen + BUF).astype(jnp.int32).reshape(2, BUF)


def draw_export_rows(key, part):
    keys = jax.random.split(jax.random.fold_in(key, 17), FRAGS)
    return jax.vmap(fragment_rows)(keys)


def with_ends(drawn, stream_key, smallest, largest):
    dims = drawn.shape
    index_at = [jax.random.randint(jax.random.fold_in(stream_key, axis), (), 0, dims[axis]) for axis in range(len(dims))]
    drawn = drawn.at[tuple(index_at)].set(smallest)
    longest = dims.index(max(dims))
    index_at[longest] = (index_at[longest] + 1) % dims[longest]
    return drawn.at[tuple(index_at)].set(largest)


def level_of(stream_key, dims, cuts, least, high):
    factor_of, own = 1.0, jax.random.fold_in(stream_key, 6)
    for axis_at, blocks in cuts:
        heights = jnp.exp(jax.random.uniform(jax.random.fold_in(own, axis_at), (blocks,), jnp.float32, least / len(cuts), high / len(cuts)))
        factor_of = factor_of * jnp.repeat(heights, dims[axis_at] // blocks).reshape([-1 if axis == axis_at else 1 for axis in range(len(dims))])
    return factor_of


def normal_values(stream_key, extent, deviation, reach, cuts=(), kind=jnp.bfloat16):
    level = level_of(stream_key, extent, cuts, -0.22, 0.18) if cuts else 1.0
    entries = jax.random.normal(stream_key, extent, jnp.float32) * deviation * level
    return jnp.minimum(jnp.maximum(entries, -reach), reach).astype(kind)


def setup_inputs(seed: int = 0) -> dict:
    streams_of = jax.random.split(jax.random.key(seed), 10)
    amps = normal_values(streams_of[0], (FRAGS, V, P_SIZE, V), 0.1, 1.5, ((0, 8), (1, 4)), jnp.float32)
    exch = normal_values(streams_of[1], (FRAGS, V, P_SIZE, V), 0.3, 4.0, ((0, 8), (1, 4)), jnp.float32)
    factors = normal_values(streams_of[2], (FRAGS, NAUX, V, V), (V * NAUX // 16) ** -0.5, 0.109375, ((0, 8), (1, 4)))
    occupied_pair_ladder = normal_values(streams_of[3], (FRAGS, P_SIZE, P_SIZE), (4 * P_SIZE) ** -0.5, 1.0, ((0, 8),), jnp.float32)
    virtual_fock_block = normal_values(streams_of[4], (FRAGS, V, V), (8 * V) ** -0.5, 0.1875, ((0, 8),), jnp.float32)
    virtual_orbital_energy = jnp.clip(1.0 + 2.0 * jax.random.uniform(streams_of[5], (FRAGS, V), jnp.float32) ** level_of(streams_of[5], (FRAGS, V), ((0, 8),), -0.2, 0.2), 1.0, 3.0)
    pair_energy = jnp.clip(-1.5 + 1.0 * jax.random.uniform(streams_of[6], (FRAGS, P_SIZE), jnp.float32) ** level_of(streams_of[6], (FRAGS, P_SIZE), ((0, 8),), -0.2, 0.2), -1.5, -0.5)
    energy_weight = with_ends(jax.random.randint(streams_of[7], (FRAGS, P_SIZE), 0, 3), jax.random.fold_in(streams_of[7], 1), 0, 2).astype(jnp.int32)
    export_rows = draw_export_rows(jax.random.fold_in(streams_of[9], 71), 0)
    return dict(amps=amps, exch=exch, factors=factors, occupied_pair_ladder=occupied_pair_ladder, virtual_fock_block=virtual_fock_block, virtual_orbital_energy=virtual_orbital_energy, pair_energy=pair_energy, energy_weight=energy_weight, export_rows=export_rows)


def ladder_term(factor_whole, cluster_amplitude):
    block_size = math.gcd(NAUX, 48)
    low_amps = lax.optimization_barrier(cluster_amplitude.astype(jnp.bfloat16)).astype(jnp.float32)
    flat_amps = low_amps.reshape(V, P_SIZE * V)
    total = jnp.zeros((V, P_SIZE, V), jnp.float32)
    for block_index in range(NAUX // block_size):
        lower_edge = block_index * block_size
        factor_block = factor_whole[lower_edge:lower_edge + block_size]
        half_done = jnp.dot(factor_block.reshape(block_size * V, V), flat_amps, preferred_element_type=jnp.float32, precision=lax.Precision.HIGHEST)
        half_done = lax.optimization_barrier(half_done.astype(jnp.bfloat16)).astype(jnp.float32)
        half_done = half_done.reshape(block_size, V, P_SIZE, V)
        total = total + jnp.einsum('qapd,qbd->apb', half_done, factor_block, precision=lax.Precision.HIGHEST)
    return total

def one_fragment(inputs):
    amps, exch, factors, occupied_pair_ladder, virtual_fock_block, virtual_orbital_energy, pair_energy = inputs
    factor_whole = factors.astype(jnp.float32)
    denominator = virtual_orbital_energy[:, None, None] + virtual_orbital_energy[None, None, :] - pair_energy[None, :, None]
    cluster_amplitude = amps
    norms = []
    for sweep_index in range(PASSES):
        ladder = ladder_term(factor_whole, cluster_amplitude)
        hole = jnp.einsum('pr,arb->apb', occupied_pair_ladder, cluster_amplitude, precision=lax.Precision.HIGHEST)
        fock_section = jnp.einsum('vn,nog->vog', virtual_fock_block, cluster_amplitude, precision=lax.Precision.HIGHEST)
        fock_section = fock_section + jnp.einsum('apc,bc->apb', cluster_amplitude, virtual_fock_block, precision=lax.Precision.HIGHEST)
        residual = exch + ladder + hole + fock_section - denominator * cluster_amplitude
        norms.append(jnp.sqrt(jnp.sum(residual * residual)))
        cluster_amplitude = cluster_amplitude + residual / denominator
    return (cluster_amplitude, jnp.stack(norms))

def pick_rows(cluster_amplitude, picked):
    return jnp.take(cluster_amplitude, picked, axis=1)

def reference(amps, exch, factors, occupied_pair_ladder, virtual_fock_block, virtual_orbital_energy, pair_energy, energy_weight, export_rows):
    all_amps, res_norms = lax.map(one_fragment, (amps, exch, factors, occupied_pair_ladder, virtual_fock_block, virtual_orbital_energy, pair_energy))
    upward = jax.vmap(pick_rows)(all_amps, export_rows[:, 0, :])
    downward = jax.vmap(pick_rows)(all_amps, export_rows[:, 1, :])
    lower = jnp.concatenate([all_amps[:1, :, :BUF], upward[:-1]], axis=0)
    upper = jnp.concatenate([downward[1:], all_amps[-1:, :, P_SIZE - BUF:]], axis=0)
    new_amps = jnp.concatenate([lower, all_amps[:, :, BUF:P_SIZE - BUF], upper], axis=2)
    weights = energy_weight.astype(jnp.float32) * 0.5
    energy = -jnp.sum(weights[:, None, :, None] * new_amps * exch) / (V * V)
    return (new_amps, res_norms, energy)
```

```python
import functools

import jax
import jax.numpy as jnp
from jax import lax
from jax.experimental import pallas as pl
from jax.experimental.pallas import tpu as pltpu
from jax.sharding import PartitionSpec as P

PASSES = 2
CHUNK = 2
AUX_BLOCK = 8
MESH = pl.DeviceIdType.MESH
NT = (((1,), (1,)), ((), ()))


def thirds(value):
    high = value.astype(jnp.bfloat16)
    rest = value - high.astype(jnp.float32)
    middle = rest.astype(jnp.bfloat16)
    return high, middle, (rest - middle.astype(jnp.float32)).astype(jnp.bfloat16)


def split_left(value):
    high, middle, small = thirds(value)
    return jnp.concatenate([high, high, middle, high, middle, small], axis=1)


def split_right(value):
    high, middle, small = thirds(value)
    return jnp.concatenate([high, middle, high, small, middle, high], axis=0)


def kernel(
    blocks,
    frags,
    amps_ref,
    exch_ref,
    factors_hbm,
    hole_ref,
    fock_ref,
    orbital_ref,
    pair_ref,
    weight_ref,
    export_ref,
    new_ref,
    norm_ref,
    energy_ref,
    fact,
    amp,
    low,
    low_t,
    half0,
    half1,
    acc,
    acc1,
    part,
    recv,
    base,
    fock_t,
    fock_col,
    row_energy,
    row_t,
    sent_rows,
    got_rows,
    sums,
    frag_sums,
    left_ref,
    right_ref,
    fact_sem,
    ag_send,
    ag_recv,
    rs_send,
    rs_recv,
    ex_send,
    ex_recv,
    sum_send,
    sum_recv,
    fs_send,
    fs_recv,
):
    me = lax.axis_index("blk")
    frag = lax.axis_index("frag")
    _, rows, pairs, virt = amps_ref.shape
    aux = fact.shape[0]
    steps = aux // AUX_BLOCK
    border = export_ref.shape[2]
    peers = [lax.rem(me + j, blocks) for j in range(1, blocks)]
    frag_peers = [lax.rem(frag + j, frags) for j in range(1, frags)]
    chunks = pairs // CHUNK
    starts = sorted(
        range(0, pairs, CHUNK), key=lambda p: p < border or p + CHUNK > pairs - border
    )
    core_chunks = sum(1 for p in starts if border <= p and p + CHUNK <= pairs - border)

    load = pltpu.make_async_copy(factors_hbm.at[0], fact, fact_sem)
    load.start()

    for p in range(pairs):
        value = amps_ref[0, :, p, :]
        amp[0, p] = value
        low[0, me, p] = value.astype(jnp.bfloat16)

    barrier = pltpu.get_barrier_semaphore()
    for peer in peers:
        pl.semaphore_signal(barrier, inc=1, device_id={"blk": peer}, device_id_type=MESH)
    for peer in frag_peers:
        pl.semaphore_signal(barrier, inc=1, device_id={"frag": peer}, device_id_type=MESH)
    pl.semaphore_wait(barrier, blocks - 1 + frags - 1)

    pending = []

    def gather(sweep, start):
        copies = []
        for j, peer in enumerate(peers):
            where = low.at[sweep, me, pl.ds(start, CHUNK)]
            copy = pltpu.make_async_remote_copy(
                src_ref=where,
                dst_ref=where,
                send_sem=ag_send.at[sweep, start // CHUNK, j],
                recv_sem=ag_recv.at[sweep, start // CHUNK, j],
                device_id={"blk": peer},
                device_id_type=MESH,
            )
            copy.start()
            copies.append(copy)
        pending.extend(copies)
        return copies

    def scatter(sweep, start):
        copies = []
        for j, peer in enumerate(peers):
            copy = pltpu.make_async_remote_copy(
                src_ref=part.at[sweep, peer, pl.ds(start, CHUNK)],
                dst_ref=recv.at[sweep, j, pl.ds(start, CHUNK)],
                send_sem=rs_send.at[sweep, start // CHUNK, j],
                recv_sem=rs_recv.at[sweep, start // CHUNK, j],
                device_id={"blk": peer},
                device_id_type=MESH,
            )
            copy.start()
            copies.append(copy)
        pending.extend(copies)
        return copies

    gathers = {(0, start): gather(0, start) for start in starts}

    offset = pl.multiple_of(me * rows, rows)
    fock_t[...] = split_right(fock_ref[0].T)
    column = lax.broadcasted_iota(jnp.int32, (virt, virt), 1)
    own = (column >= offset) & (column < offset + rows)
    fock_col[...] = split_left(jnp.where(own, fock_ref[0], 0.0))
    row_t[...] = jnp.broadcast_to(orbital_ref[...], (virt, virt)).T
    row_energy[...] = row_t[pl.ds(offset, rows), :] + orbital_ref[...]

    def make_base(sweep):
        def product(p, carry):
            right_ref[p] = jnp.dot(
                split_left(amp[sweep, p]), fock_t[...], preferred_element_type=jnp.float32
            )
            return carry

        lax.fori_loop(0, pairs, product, 0)
        for p in range(pairs):
            total = exch_ref[0, :, p, :] + right_ref[p]
            for r in range(pairs):
                total = total + hole_ref[0, p, r] * amp[sweep, r]
            total = total - (row_energy[...] - pair_ref[0, p]) * amp[sweep, p]
            base[sweep, p] = total

    make_base(0)
    load.wait()

    def first_half(index, half):
        at = pl.multiple_of(index * AUX_BLOCK, AUX_BLOCK)
        slab = fact[pl.ds(at, AUX_BLOCK)].reshape(AUX_BLOCK * virt, virt)
        done = lax.dot_general(
            low_t[...], slab, NT, preferred_element_type=jnp.float32
        ).astype(jnp.bfloat16)
        for q in range(AUX_BLOCK):
            for p in range(CHUNK):
                half[q * virt : (q + 1) * virt, p * virt : (p + 1) * virt] = done[
                    p * virt : (p + 1) * virt, q * virt : (q + 1) * virt
                ]

    def second_half(index, half, acc):
        at = pl.multiple_of(index * AUX_BLOCK, AUX_BLOCK)
        slab = jnp.concatenate([fact[at + q] for q in range(AUX_BLOCK)], axis=1)
        acc[...] += jnp.dot(slab, half[...], preferred_element_type=jnp.float32)

    def compute(sweep, start):
        for i in range(CHUNK):
            whole = low[sweep, :, start + i].reshape(virt, virt)
            low_t[i * virt : (i + 1) * virt, :] = whole.T
        acc[...] = jnp.zeros_like(acc)
        acc1[...] = jnp.zeros_like(acc1)
        first_half(0, half0)

        def body(i, carry):
            second_half(2 * i, half0, acc)
            first_half(2 * i + 1, half1)
            second_half(2 * i + 1, half1, acc1)
            first_half(jnp.minimum(2 * i + 2, steps - 1), half0)
            return carry

        lax.fori_loop(0, steps // 2, body, 0)
        def left(i, carry):
            whole = jnp.concatenate([amp[sweep, start + i]] * blocks, axis=0)
            left_ref[i] = jnp.dot(
                fock_col[...], split_right(whole), preferred_element_type=jnp.float32
            )
            return carry

        lax.fori_loop(0, CHUNK, left, 0)
        for i in range(CHUNK):
            cols = slice(i * virt, (i + 1) * virt)
            total = (acc[:, cols] + acc1[:, cols]).T + left_ref[i]
            for k in range(blocks):
                part[sweep, k, start + i] = total[k * rows : (k + 1) * rows]

    norm_sums = [jnp.zeros((8, virt), jnp.float32) for _ in range(PASSES)]

    def finish(sweep, start, copies):
        for copy in copies:
            copy.wait_recv()
        for p in range(start, start + CHUNK):
            residual = base[sweep, p] + part[sweep, me, p]
            for j in range(blocks - 1):
                residual = residual + recv[sweep, j, p]
            norm_sums[sweep] += jnp.sum((residual * residual).reshape(rows // 8, 8, virt), axis=0)
            value = amp[sweep, p] + residual / (row_energy[...] - pair_ref[0, p])
            amp[sweep + 1, p] = value
            if sweep + 1 < PASSES:
                low[sweep + 1, me, p] = value.astype(jnp.bfloat16)
        if sweep + 1 < PASSES:
            gathers[sweep + 1, start] = gather(sweep + 1, start)
        if start == starts[-1] and sweep + 1 < PASSES:
            make_base(sweep + 1)

    exports = []

    def export():
        for side, target in ((0, lax.rem(frag + 1, frags)), (1, lax.rem(frag + frags - 1, frags))):
            for r in range(border):
                sent_rows[side, r] = amp[PASSES, export_ref[0, side, r]]
            copy = pltpu.make_async_remote_copy(
                src_ref=sent_rows.at[side],
                dst_ref=got_rows.at[side],
                send_sem=ex_send.at[side],
                recv_sem=ex_recv.at[side],
                device_id={"frag": target},
                device_id_type=MESH,
            )
            copy.start()
            exports.append(copy)
        pending.extend(exports)

    waiting = None
    finished = 0
    for sweep in range(PASSES):
        for start in starts:
            for copy in gathers[sweep, start]:
                copy.wait_recv()
            compute(sweep, start)
            copies = scatter(sweep, start)
            if waiting is not None:
                finish(*waiting)
                if waiting[0] == PASSES - 1:
                    finished += 1
                    if finished == core_chunks:
                        export()
            waiting = (sweep, start, copies)
    finish(*waiting)

    for copy in exports:
        copy.wait_recv()
    energy = jnp.zeros((8, virt), jnp.float32)
    for p in range(pairs):
        value = amp[PASSES, p]
        if p < border:
            value = jnp.where(frag > 0, got_rows[0, p], value)
        if p >= pairs - border:
            value = jnp.where(frag < frags - 1, got_rows[1, p - (pairs - border)], value)
        new_ref[0, :, p, :] = value
        product = jnp.sum((value * exch_ref[0, :, p, :]).reshape(rows // 8, 8, virt), axis=0)
        energy = energy + (weight_ref[0, p].astype(jnp.float32) * 0.5) * product

    for s in range(PASSES):
        sums[me, s] = norm_sums[s]
    sums[me, PASSES] = energy
    copies = []
    for j, peer in enumerate(peers):
        copy = pltpu.make_async_remote_copy(
            src_ref=sums.at[me],
            dst_ref=sums.at[me],
            send_sem=sum_send.at[j],
            recv_sem=sum_recv.at[j],
            device_id={"blk": peer},
            device_id_type=MESH,
        )
        copy.start()
        copies.append(copy)
    for copy in copies:
        copy.wait_recv()
    pending.extend(copies)
    totals = jnp.sum(sums[...], axis=0)
    frag_sums[frag] = totals[PASSES]
    copies = []
    for j, peer in enumerate(frag_peers):
        copy = pltpu.make_async_remote_copy(
            src_ref=frag_sums.at[frag],
            dst_ref=frag_sums.at[frag],
            send_sem=fs_send.at[j],
            recv_sem=fs_recv.at[j],
            device_id={"frag": peer},
            device_id_type=MESH,
        )
        copy.start()
        copies.append(copy)
    norms = [jnp.sqrt(jnp.sum(jnp.sum(totals[s], axis=0, keepdims=True), axis=1, keepdims=True)) for s in range(PASSES)]
    lane = lax.broadcasted_iota(jnp.int32, (1, PASSES), 1)
    line = jnp.zeros((1, PASSES), jnp.float32)
    for s in range(PASSES):
        line = jnp.where(lane == s, norms[s], line)
    norm_ref[...] = line
    for copy in copies:
        copy.wait_recv()
    pending.extend(copies)
    whole = jnp.sum(frag_sums[...], axis=0)
    energy_ref[...] = -jnp.sum(jnp.sum(whole, axis=0, keepdims=True), axis=1, keepdims=True) / (virt * virt)
    for copy in pending:
        copy.wait_send()


def on_device(blocks, frags, *args):
    amps, _, factors = args[:3]
    _, rows, pairs, virt = amps.shape
    aux = factors.shape[1]
    border = args[-1].shape[2]
    chunks = pairs // CHUNK
    vmem = pl.BlockSpec(memory_space=pltpu.VMEM)
    smem = pl.BlockSpec(memory_space=pltpu.SMEM)
    f32, bf16 = jnp.float32, jnp.bfloat16
    dma = pltpu.SemaphoreType.DMA
    new_amps, norms, energy = pl.pallas_call(
        functools.partial(kernel, blocks, frags),
        out_shape=(
            jax.ShapeDtypeStruct(amps.shape, f32),
            jax.ShapeDtypeStruct((1, PASSES), f32),
            jax.ShapeDtypeStruct((1, 1), f32),
        ),
        in_specs=[
            vmem,
            vmem,
            pl.BlockSpec(memory_space=pl.ANY),
            smem,
            vmem,
            vmem,
            smem,
            smem,
            smem,
        ],
        out_specs=(vmem, vmem, vmem),
        scratch_shapes=[
            pltpu.VMEM((aux, virt, virt), bf16),
            pltpu.VMEM((PASSES + 1, pairs, rows, virt), f32),
            pltpu.VMEM((PASSES, blocks, pairs, rows, virt), bf16),
            pltpu.VMEM((CHUNK * virt, virt), bf16),
            pltpu.VMEM((AUX_BLOCK * virt, CHUNK * virt), bf16),
            pltpu.VMEM((AUX_BLOCK * virt, CHUNK * virt), bf16),
            pltpu.VMEM((virt, CHUNK * virt), f32),
            pltpu.VMEM((virt, CHUNK * virt), f32),
            pltpu.VMEM((PASSES, blocks, pairs, rows, virt), f32),
            pltpu.VMEM((PASSES, blocks - 1, pairs, rows, virt), f32),
            pltpu.VMEM((PASSES, pairs, rows, virt), f32),
            pltpu.VMEM((6 * virt, virt), bf16),
            pltpu.VMEM((virt, 6 * virt), bf16),
            pltpu.VMEM((rows, virt), f32),
            pltpu.VMEM((virt, virt), f32),
            pltpu.VMEM((2, border, rows, virt), f32),
            pltpu.VMEM((2, border, rows, virt), f32),
            pltpu.VMEM((blocks, PASSES + 1, 8, virt), f32),
            pltpu.VMEM((frags, 8, virt), f32),
            pltpu.VMEM((CHUNK, virt, virt), f32),
            pltpu.VMEM((pairs, rows, virt), f32),
            dma,
            dma((PASSES, chunks, blocks - 1)),
            dma((PASSES, chunks, blocks - 1)),
            dma((PASSES, chunks, blocks - 1)),
            dma((PASSES, chunks, blocks - 1)),
            dma((2,)),
            dma((2,)),
            dma((blocks - 1,)),
            dma((blocks - 1,)),
            dma((frags - 1,)),
            dma((frags - 1,)),
        ],
        compiler_params=pltpu.CompilerParams(
            collective_id=0, has_side_effects=True, vmem_limit_bytes=48 * 2**20
        ),
    )(*args)
    return new_amps, norms, energy.reshape(())


def solution(mesh):
    placed = (
        P("frag", "blk", None, None),
        P("frag", "blk", None, None),
        P("frag", "blk", None, None),
        P("frag", None, None),
        P("frag", None, None),
        P("frag", None),
        P("frag", None),
        P("frag", None),
        P("frag", None, None),
    )
    return jax.shard_map(
        functools.partial(on_device, mesh.shape["blk"], mesh.shape["frag"]),
        mesh=mesh,
        in_specs=placed,
        out_specs=(P("frag", "blk", None, None), P("frag", None), P()),
        check_vma=False,
    )
```
